32 devices in a mesh: gy: 8 (over z, x), gz: 4 (over y, core).
Axes of the slice: x: 2, y: 2, z: 4, core: 2. Of those that a mesh axis runs over, the one named last changes fastest.
Arguments:
- fraction: float32 [64, 64, 1024], P('gz', 'gy'), may hold values from 0 to 1
- velocity_x: float32 [64, 64, 1024], P('gz', 'gy'), may hold values from -9 to 9
- velocity_y: float32 [64, 64, 1024], P('gz', 'gy'), may hold values from -9 to 9
- velocity_z: float32 [64, 64, 1024], P('gz', 'gy'), may hold values from -9 to 9
Outputs:
- advected: float32 [64, 64, 1024], P('gz', 'gy')
- time_step: float32 [], replicated
The draws below stay inside these ranges and needn't reach their ends.
All inputs are finite; a program needn't handle non-finite values. Where the reference program divides by a largest or mean magnitude, that divisor is 1e-20 or more.
Results may differ from the reference program's by a relative error of at most 0.0003.
Values sent between devices are 32-bit elements; how exact they have to be, the bound alone decides.
A program may use at most 64 MiB of HBM per device.

```python
import jax
import jax.numpy as jnp

NX = 1024
CY = 8
CZ = 16
NEWTON = 5
NY = 64
NZ = 64
N_GY = 8
N_GZ = 4


def block_linear():
    plane_owner = jnp.arange(NZ) // CZ
    row_owner = jnp.arange(NY) // CY
    return row_owner[None, :] * N_GZ + plane_owner[:, None]


def spread_blocks(values):
    return values[block_linear()][:, :, None]


def draw_fraction(key, part):
    key_pick, key_coin, key_value, key_level, key_jitter, key_power = jax.random.split(key, 6)
    count = N_GY * N_GZ
    linear = jnp.arange(count).astype(jnp.float32)
    rise = 0.5 + linear / (count - 1)
    level = jax.random.uniform(key_level, (), jnp.float32, 0.15, 0.45)
    jitter = jnp.exp(jax.random.uniform(key_jitter, (count,), jnp.float32, jnp.log(0.6), jnp.log(1.4)))
    mixed_rate = spread_blocks(level * rise * jitter)
    power = jax.random.uniform(key_power, (count,), jnp.float32, 1.0, 2.0)
    chooser = jax.random.uniform(key_pick, (NZ, NY, NX), jnp.float32)
    pure_value = (jax.random.uniform(key_coin, (NZ, NY, NX), jnp.float32) < 0.5).astype(jnp.float32)
    mixture = jax.random.uniform(key_value, (NZ, NY, NX), jnp.float32)
    mixture = jnp.power(mixture, spread_blocks(power))
    return jnp.where(chooser < mixed_rate, mixture, pure_value)


def speed_field(key, which):
    local_key = jax.random.fold_in(key, which)
    key_values, key_peak, key_lower, key_upper = jax.random.split(local_key, 4)
    count = N_GY * N_GZ
    half = count // 2
    ranks = jnp.concatenate([jax.random.permutation(key_lower, half), half + jax.random.permutation(key_upper, count - half)]).astype(jnp.float32)
    peak = jax.random.uniform(key_peak, (), jnp.float32, 3.0, 9.0)
    amplitude = peak * (1.0 + 2.0 * ranks / (count - 1)) / 3.0
    values = jnp.clip(jax.random.normal(key_values, (NZ, NY, NX), jnp.float32), -3.0, 3.0) / 3.0
    return values * spread_blocks(amplitude)


def draw_velocity_x(key, part):
    return speed_field(key, 11)


def draw_velocity_y(key, part):
    return speed_field(key, 23)


def draw_velocity_z(key, part):
    return speed_field(key, 37)


def setup_inputs(seed: int = 0) -> dict:
    key_of = jax.random.split(jax.random.key(seed), 5)
    fraction = draw_fraction(jax.random.fold_in(key_of[4], 71), 0)
    velocity_x = draw_velocity_x(jax.random.fold_in(key_of[4], 71), 0)
    velocity_y = draw_velocity_y(jax.random.fold_in(key_of[4], 71), 0)
    velocity_z = draw_velocity_z(jax.random.fold_in(key_of[4], 71), 0)
    return dict(fraction=fraction, velocity_x=velocity_x, velocity_y=velocity_y, velocity_z=velocity_z)


tilt_floor = 0.1
courant = 0.45
epsilon = 1e-6


def cube_step(reach, height):
    safe = jnp.where(height > 0, height, 1.0)
    whole = 3.0 * reach * reach - 3.0 * reach * height + height * height
    partial_part = reach * reach * reach / safe
    return jnp.where(reach - height >= 0, whole, jnp.where(reach >= 0, partial_part, 0.0))


def cube_rate(reach, height):
    safe = jnp.where(height > 0, height, 1.0)
    whole = 6.0 * reach - 3.0 * height
    partial_part = 3.0 * reach * reach / safe
    return jnp.where(reach - height >= 0, whole, jnp.where(reach >= 0, partial_part, 0.0))


def region_volume(offset, tilt_a, tilt_b, height, extent):
    combo = cube_step(offset, height) - cube_step(offset - tilt_a, height) - cube_step(offset - tilt_b, height) + cube_step(offset - tilt_a - tilt_b, height)
    return extent * combo / (6.0 * tilt_a * tilt_b)


def section_area(offset, tilt_a, tilt_b, height):
    combo = cube_rate(offset, height) - cube_rate(offset - tilt_a, height) - cube_rate(offset - tilt_b, height) + cube_rate(offset - tilt_a - tilt_b, height)
    return combo / (6.0 * tilt_a * tilt_b)


def youngs_slope(padded):
    def smooth_zero(arr):
        return arr[:-2] + 2.0 * arr[1:-1] + arr[2:]

    def smooth_one(arr):
        return arr[:, :-2] + 2.0 * arr[:, 1:-1] + arr[:, 2:]

    def smooth_cells(arr):
        return jnp.roll(arr, 1, 2) + 2.0 * arr + jnp.roll(arr, -1, 2)

    diff_zero = padded[2:] - padded[:-2]
    diff_one = padded[:, 2:] - padded[:, :-2]
    diff_cells = jnp.roll(padded, -1, 2) - jnp.roll(padded, 1, 2)
    grad_zero = smooth_cells(smooth_one(diff_zero)) / 32.0
    grad_one = smooth_cells(smooth_zero(diff_one)) / 32.0
    grad_cells = smooth_one(smooth_zero(diff_cells)) / 32.0
    return (grad_zero, grad_one, grad_cells)


def plane_for(fraction, slopes, axis_dim):
    slope_d = slopes[axis_dim]
    across = [slopes[index] for index in range(3) if index != axis_dim]
    tilt_d = jnp.abs(slope_d)
    tilt_a = jnp.abs(across[0]) + tilt_floor
    tilt_b = jnp.abs(across[1]) + tilt_floor
    volume = jnp.clip(fraction, 0.0, 1.0)
    lesser = jnp.minimum(volume, 1.0 - volume)
    summed = tilt_a + tilt_b + tilt_d
    offset = 0.5 * summed
    for repeat in range(NEWTON):
        offset = offset - (region_volume(offset, tilt_a, tilt_b, tilt_d, 1.0) - lesser) / section_area(offset, tilt_a, tilt_b, tilt_d)
    offset = jnp.where(volume > 0.5, summed - offset, offset)
    return (offset, tilt_a, tilt_b, tilt_d, slope_d > 0)


def outflow(planes, width, upward):
    offset, tilt_a, tilt_b, tilt_d, mirrored = planes
    if upward:
        start_at = jnp.where(mirrored, 0.0, 1.0 - width)
    else:
        start_at = jnp.where(mirrored, 1.0 - width, 0.0)
    return region_volume(offset - tilt_d * start_at, tilt_a, tilt_b, tilt_d * width, width)


def sweep(fraction, velocity, axis_dim, time_step):
    padded = jnp.pad(fraction, ((1, 1), (1, 1), (0, 0)), mode="wrap")
    planes = plane_for(fraction, youngs_slope(padded), axis_dim)
    velocity_low = jnp.roll(velocity, 1, axis_dim)
    out_upper = outflow(planes, jnp.maximum(time_step * velocity, 0.0), True)
    out_lower = outflow(planes, jnp.maximum(-time_step * velocity_low, 0.0), False)
    from_below = jnp.roll(out_upper, 1, axis_dim)
    from_above = jnp.roll(out_lower, -1, axis_dim)
    divisor = 1.0 - time_step * velocity + time_step * velocity_low
    return (fraction - out_upper - out_lower + from_below + from_above) / divisor


def reference(fraction, velocity_x, velocity_y, velocity_z):
    umax = jnp.maximum(jnp.maximum(jnp.max(jnp.abs(velocity_x)), jnp.max(jnp.abs(velocity_y))), jnp.max(jnp.abs(velocity_z)))
    share = jnp.sum(4.0 * fraction * (1.0 - fraction)) / (NX * NY * NZ)
    time_step = courant / ((umax + epsilon) * (1.0 + share))
    field = sweep(fraction, velocity_x, 2, time_step)
    field = sweep(field, velocity_y, 1, time_step)
    field = sweep(field, velocity_z, 0, time_step)
    return field, time_step
```

```python
import functools

import jax
import jax.numpy as jnp
from jax import lax
from jax.experimental import pallas as pl
from jax.experimental.pallas import tpu as pltpu
from jax.sharding import PartitionSpec as P

NEWTON = 5
LANES = 128

tilt_floor = 0.1
courant = 0.45
epsilon = 1e-06
tiny = 1e-30

MESH = pl.DeviceIdType.MESH
SIDES = [(a, b) for a in (-1, 0, 1) for b in (-1, 0, 1) if (a, b) != (0, 0)]


def lane_of(value):
    return lax.broadcasted_iota(jnp.int32, value.shape, value.ndim - 1)


def x_next(value):
    turned = pltpu.roll(value, LANES - 1, value.ndim - 1)
    carried = pltpu.roll(turned, value.shape[-2] - 1, value.ndim - 2)
    return jnp.where(lane_of(value) == LANES - 1, carried, turned)


def x_prev(value):
    turned = pltpu.roll(value, 1, value.ndim - 1)
    carried = pltpu.roll(turned, 1, value.ndim - 2)
    return jnp.where(lane_of(value) == 0, carried, turned)


def solve_offset(g, tilt_a, tilt_b, tilt_d):
    volume = jnp.clip(g, 0.0, 1.0)
    lesser = jnp.minimum(volume, 1.0 - volume)
    low = jnp.minimum(tilt_a, tilt_b)
    high = jnp.maximum(tilt_a, tilt_b)
    n1 = jnp.minimum(low, tilt_d)
    middle = jnp.maximum(low, tilt_d)
    n2 = jnp.minimum(middle, high)
    n3 = jnp.maximum(middle, high)
    summed = tilt_a + tilt_b + tilt_d
    inverse = 1.0 / jnp.maximum(n1, tiny)
    third = inverse * (1.0 / 3.0)
    product = n2 * n3
    target = 2.0 * product * lesser
    gap = jnp.maximum(n1 + n2 - n3, 0.0)
    rate = 2.0 * n2 - 0.5 * gap * (gap * inverse)
    offset = 0.5 * summed - (product - target) / rate
    for repeat in range(NEWTON - 1):
        p1 = jnp.minimum(offset, n1)
        q1 = offset - p1
        m2 = jnp.maximum(offset - n2, 0.0)
        p2 = jnp.minimum(m2, n1)
        q2 = m2 - p2
        p3 = jnp.minimum(jnp.maximum(offset - n3, 0.0), n1)
        s1, s2, s3 = p1 * p1, p2 * p2, p3 * p3
        squares = s1 - s2 - s3
        cubes = s1 * p1 - s2 * p2 - s3 * p3
        q = q1 - q2
        rate = squares * inverse + (q + q)
        volume_part = cubes * third + q * (q1 + q2 + n1)
        offset = offset - (volume_part - target) / rate
    return jnp.where(volume > 0.5, summed - offset, offset)


def face_flux(cross, offset, tilt_a, tilt_b, slope):
    turn = slope * cross
    height = jnp.abs(turn)
    reach = offset - jnp.where(turn > 0, 0.0, jnp.abs(slope) - height)

    def parts(value):
        inside = jnp.maximum(value, 0.0)
        p = jnp.minimum(inside, height)
        q = inside - p
        return p * p * p, q * (q + height)

    reach_a = reach - tilt_a
    p0, q0 = parts(reach)
    p1, q1 = parts(reach_a)
    p2, q2 = parts(reach - tilt_b)
    p3, q3 = parts(reach_a - tilt_b)
    cubes = (p0 - p1) - (p2 - p3)
    wholes = (q0 - q1) - (q2 - q3)
    combo = cubes * ((1.0 / 3.0) / jnp.maximum(height, tiny)) + wholes
    return cross * combo / (2.0 * tilt_a * tilt_b)


def kernel(
    n_gy, n_gz, f_ref, vx_ref, vy_ref, vz_ref, out_ref, dt_ref,
    g0, g1, g2, sx, dx, off, ta, tb, sd, vx, vy, vz, fy, fz,
    fy_in, fz_in, part_y, part_z,
    halo_send, halo_recv, vel_send, vel_recv, flux_send, flux_recv,
    py_send, py_recv, pz_send, pz_recv,
):
    Z = f_ref.shape[0]
    T = sx.shape[2]
    Y = f_ref.shape[1] // T
    my = lax.axis_index("gy")
    mz = lax.axis_index("gz")

    def at(dz, dy):
        return {
            "gy": lax.rem(my + dy + n_gy, n_gy),
            "gz": lax.rem(mz + dz + n_gz, n_gz),
        }

    barrier = pltpu.get_barrier_semaphore()
    greeted = [(0, i) for i in range(1, n_gy)] + [(i, 0) for i in range(1, n_gz)]
    greeted += [(a, b) for a in (-1, 1) for b in (-1, 1)]
    for dz, dy in greeted:
        pl.semaphore_signal(barrier, inc=1, device_id=at(dz, dy), device_id_type=MESH)

    def rows_of(ref, z, y):
        return ref[z, pl.ds(y, T, stride=Y), :]

    def loop(low, high, body):
        def step(i, carry):
            body(i)
            return carry
        lax.fori_loop(low, high, step, 0)

    def span(side, count):
        if side == 0:
            return pl.ds(1, count), pl.ds(1, count)
        if side > 0:
            return pl.ds(count, 1), pl.ds(0, 1)
        return pl.ds(1, 1), pl.ds(count + 1, 1)

    def halo_copies(g, which):
        copies = []
        for index, (dz, dy) in enumerate(SIDES):
            src_z, dst_z = span(dz, Z)
            src_y, dst_y = span(dy, Y)
            copies.append(pltpu.make_async_remote_copy(
                src_ref=g.at[src_z, src_y],
                dst_ref=g.at[dst_z, dst_y],
                send_sem=halo_send.at[which, index],
                recv_sem=halo_recv.at[which, index],
                device_id=at(dz, dy),
                device_id_type=MESH,
            ))
        return copies

    def fill(z, total):
        for y in range(Y):
            f = rows_of(f_ref, z, y)
            g0[z + 1, y + 1] = f
            total = total + 4.0 * f * (1.0 - f)
        return total

    total = lax.fori_loop(0, Z, fill, jnp.zeros((T, LANES), jnp.float32))
    pl.semaphore_wait(barrier, len(greeted))
    halos0 = halo_copies(g0, 0)
    for copy in halos0:
        copy.start()

    def fill_velocity(z, peak):
        for y in range(Y):
            a = rows_of(vx_ref, z, y)
            b = rows_of(vy_ref, z, y)
            c = rows_of(vz_ref, z, y)
            vx[z, y] = a
            vy[z, y + 1] = b
            vz[z + 1, y] = c
            peak = jnp.maximum(peak, jnp.maximum(jnp.abs(a), jnp.maximum(jnp.abs(b), jnp.abs(c))))
        return peak

    peak = lax.fori_loop(0, Z, fill_velocity, jnp.zeros((T, LANES), jnp.float32))
    part_y[my, 0] = total
    part_y[my, 1] = peak
    vel_copies = [
        pltpu.make_async_remote_copy(
            src_ref=vy.at[:, pl.ds(Y, 1)], dst_ref=vy.at[:, pl.ds(0, 1)],
            send_sem=vel_send.at[0], recv_sem=vel_recv.at[0],
            device_id=at(0, 1), device_id_type=MESH,
        ),
        pltpu.make_async_remote_copy(
            src_ref=vz.at[pl.ds(Z, 1)], dst_ref=vz.at[pl.ds(0, 1)],
            send_sem=vel_send.at[1], recv_sem=vel_recv.at[1],
            device_id=at(1, 0), device_id_type=MESH,
        ),
    ]

    def part_copies(part, mine, send, recv, count, along_y):
        copies = []
        for i in range(1, count):
            copies.append(pltpu.make_async_remote_copy(
                src_ref=part.at[mine], dst_ref=part.at[mine],
                send_sem=send.at[i - 1], recv_sem=recv.at[i - 1],
                device_id=at(0, i) if along_y else at(i, 0), device_id_type=MESH,
            ))
        return copies

    y_parts = part_copies(part_y, my, py_send, py_recv, n_gy, True)
    for copy in y_parts:
        copy.start()
    for copy in vel_copies:
        copy.start()

    def smooth_rows(g, z, y, kz, ky):
        value = g[pl.ds(z, kz), pl.ds(y, ky)]
        after, before = x_next(value), x_prev(value)
        sx[pl.ds(z, kz), pl.ds(y, ky)] = before + (value + value) + after
        dx[pl.ds(z, kz), pl.ds(y, ky)] = after - before

    def smooth_inside(g):
        loop(1, Z + 1, lambda z: smooth_rows(g, z, 1, 1, Y))

    def smooth_ghosts(g):
        smooth_rows(g, 0, 0, 1, Y + 2)
        smooth_rows(g, Z + 1, 0, 1, Y + 2)

        def edge(z):
            smooth_rows(g, z, 0, 1, 1)
            smooth_rows(g, z, Y + 1, 1, 1)
        loop(1, Z + 1, edge)

    def smooth_zero(arr):
        mid = arr[1:-1]
        return (arr[:-2] + mid) + (mid + arr[2:])

    def smooth_one(arr):
        mid = arr[:, 1:-1]
        return (arr[:, :-2] + mid) + (mid + arr[:, 2:])

    def plane(g, dim, z, y, kz, ky):
        s = sx[pl.ds(z, kz + 2), pl.ds(y, ky + 2)]
        d = dx[pl.ds(z, kz + 2), pl.ds(y, ky + 2)]
        grad_zero = smooth_one(s[2:] - s[:-2]) * (1.0 / 32.0)
        across = smooth_zero(s)
        grad_one = (across[:, 2:] - across[:, :-2]) * (1.0 / 32.0)
        grad_cells = smooth_one(smooth_zero(d)) * (1.0 / 32.0)
        slopes = (grad_zero, grad_one, grad_cells)
        slope = slopes[dim]
        tilt_a, tilt_b = [jnp.abs(slopes[e]) + tilt_floor for e in range(3) if e != dim]
        value = g[pl.ds(z + 1, kz), pl.ds(y + 1, ky)]
        where = (pl.ds(z, kz), pl.ds(y, ky))
        off[where] = solve_offset(value, tilt_a, tilt_b, jnp.abs(slope))
        ta[where] = tilt_a
        tb[where] = tilt_b
        sd[where] = slope

    half = (Y - 2) // 2
    quarter = Y // 2

    def planes_inside(g, dim, low, high):
        def body(z):
            plane(g, dim, z, 1, 1, half)
            plane(g, dim, z, 1 + half, 1, Y - 2 - half)
        loop(low, high, body)

    def planes_edge(g, dim):
        for_rows_edge(lambda z, y, kz, ky: plane(g, dim, z, y, kz, ky))

    def for_rows_edge(body):
        def ends(i):
            z = i * (Z - 1)
            body(z, 0, 1, quarter)
            body(z, quarter, 1, Y - quarter)
        loop(0, 2, ends)

        def sides(i):
            z = 1 + 2 * i
            body(z, 0, 2, 1)
            body(z, Y - 1, 2, 1)
        loop(0, (Z - 2) // 2, sides)

    def for_rows_inside(body):
        def step(z):
            body(z, 1, 1, half)
            body(z, 1 + half, 1, Y - 2 - half)
        loop(1, Z - 1, step)

    def for_rows(body):
        def step(z):
            body(z, 0, 1, quarter)
            body(z, quarter, 1, Y - quarter)
        loop(0, Z, step)

    smooth_inside(g0)
    planes_inside(g0, 2, 1, Z // 2)
    for copy in y_parts:
        copy.wait()
    sums = part_y[0, 0]
    peaks = part_y[0, 1]
    for i in range(1, n_gy):
        sums = sums + part_y[i, 0]
        peaks = jnp.maximum(peaks, part_y[i, 1])
    part_z[mz, 0] = sums
    part_z[mz, 1] = peaks
    z_parts = part_copies(part_z, mz, pz_send, pz_recv, n_gz, False)
    for copy in z_parts:
        copy.start()
    planes_inside(g0, 2, Z // 2, Z - 1)
    for copy in halos0:
        copy.wait()
    smooth_ghosts(g0)
    planes_edge(g0, 2)
    for copy in z_parts:
        copy.wait()
    sums = part_z[0, 0]
    peaks = part_z[0, 1]
    for i in range(1, n_gz):
        sums = sums + part_z[i, 0]
        peaks = jnp.maximum(peaks, part_z[i, 1])
    cells_all = float(Z * Y * T * LANES * n_gy * n_gz)
    share = jnp.broadcast_to(jnp.sum(sums, keepdims=True), (T, LANES)) / cells_all
    umax = jnp.broadcast_to(jnp.max(peaks, keepdims=True), (T, LANES))
    step_value = courant / ((umax + epsilon) * (1.0 + share))
    dt_ref[0, 0] = jnp.max(step_value)
    dt = step_value[None, None]

    def x_update(z, y, kz, ky):
        where = (pl.ds(z, kz), pl.ds(y, ky))
        cross = dt * vx[where]
        upward = cross > 0

        def donor(ref):
            value = ref[where]
            return jnp.where(upward, value, x_next(value))

        flux = face_flux(cross, donor(off), donor(ta), donor(tb), donor(sd))
        value = g0[pl.ds(z + 1, kz), pl.ds(y + 1, ky)]
        g1[pl.ds(z + 1, kz), pl.ds(y + 1, ky)] = (value - flux + x_prev(flux)) / (
            1.0 - cross + x_prev(cross)
        )

    for_rows_edge(x_update)
    halos1 = halo_copies(g1, 1)
    for copy in halos1:
        copy.start()
    for_rows_inside(x_update)
    for copy in vel_copies:
        copy.wait()

    smooth_inside(g1)
    planes_inside(g1, 1, 1, Z - 1)
    for copy in halos1:
        copy.wait()
    smooth_ghosts(g1)
    planes_edge(g1, 1)

    def own_flux(velocity, where, at_face, least):
        cross = dt * velocity[at_face]
        cross = jnp.minimum(cross, 0.0) if least else jnp.maximum(cross, 0.0)
        return face_flux(cross, off[where], ta[where], tb[where], sd[where])

    def y_ends(i):
        rows = pl.ds(2 * i, 2)
        first, last = pl.ds(0, 1), pl.ds(Y - 1, 1)
        fy[rows, first] = own_flux(vy, (rows, first), (rows, first), True)
        fy[rows, pl.ds(Y, 1)] = own_flux(vy, (rows, last), (rows, pl.ds(Y, 1)), False)
    loop(0, Z // 2, y_ends)

    def flux_copies(flux, arrived, which, spans, steps):
        copies = []
        for i in range(2):
            copies.append(pltpu.make_async_remote_copy(
                src_ref=flux.at[spans[i]],
                dst_ref=arrived.at[i],
                send_sem=flux_send.at[which, i], recv_sem=flux_recv.at[which, i],
                device_id=at(*steps[i]), device_id_type=MESH,
            ))
        return copies

    every = pl.ds(0, Z)
    y_flux = flux_copies(
        fy, fy_in, 0, [(every, pl.ds(Y, 1)), (every, pl.ds(0, 1))], [(0, 1), (0, -1)]
    )
    for copy in y_flux:
        copy.start()

    def between(velocity, at_face, below, above):
        cross = dt * velocity[at_face]
        upward = cross > 0

        def donor(ref):
            return jnp.where(upward, ref[below], ref[above])

        return face_flux(cross, donor(off), donor(ta), donor(tb), donor(sd))

    def y_inside(z):
        rows = pl.ds(z, 1)
        for low, count in ((1, half), (1 + half, Y - 1 - half)):
            fy[rows, pl.ds(low, count)] = between(
                vy, (rows, pl.ds(low, count)), (rows, pl.ds(low - 1, count)), (rows, pl.ds(low, count))
            )
    loop(0, Z, y_inside)
    for copy in y_flux:
        copy.wait()

    def y_merge(i):
        rows = pl.ds(4 * i, 4)
        fy[rows, pl.ds(0, 1)] = fy[rows, pl.ds(0, 1)] + fy_in[0, rows]
        fy[rows, pl.ds(Y, 1)] = fy[rows, pl.ds(Y, 1)] + fy_in[1, rows]
    loop(0, Z // 4, y_merge)

    def y_update(z, y, kz, ky):
        rows = pl.ds(z, kz)
        low, high = pl.ds(y, ky), pl.ds(y + 1, ky)
        inside = (pl.ds(z + 1, kz), pl.ds(y + 1, ky))
        g2[inside] = (g1[inside] - fy[rows, high] + fy[rows, low]) / (
            1.0 - dt * vy[rows, high] + dt * vy[rows, low]
        )

    for_rows_edge(y_update)
    halos2 = halo_copies(g2, 2)
    for copy in halos2:
        copy.start()
    for_rows_inside(y_update)

    smooth_inside(g2)
    planes_inside(g2, 0, 1, Z - 1)
    for copy in halos2:
        copy.wait()
    smooth_ghosts(g2)
    planes_edge(g2, 0)

    def z_ends(i):
        cols = pl.ds(2 * i, 2)
        first, last = pl.ds(0, 1), pl.ds(Z - 1, 1)
        fz[first, cols] = own_flux(vz, (first, cols), (first, cols), True)
        fz[pl.ds(Z, 1), cols] = own_flux(vz, (last, cols), (pl.ds(Z, 1), cols), False)
    loop(0, Y // 2, z_ends)
    z_flux = flux_copies(fz, fz_in, 1, [(pl.ds(Z, 1),), (pl.ds(0, 1),)], [(1, 0), (-1, 0)])
    for copy in z_flux:
        copy.start()

    def z_inside(z):
        face, below = pl.ds(z, 1), pl.ds(z - 1, 1)
        for low, count in ((0, quarter), (quarter, Y - quarter)):
            cols = pl.ds(low, count)
            fz[face, cols] = between(vz, (face, cols), (below, cols), (face, cols))
    loop(1, Z, z_inside)
    for copy in z_flux:
        copy.wait()
    fz[pl.ds(0, 1)] = fz[pl.ds(0, 1)] + fz_in[0]
    fz[pl.ds(Z, 1)] = fz[pl.ds(Z, 1)] + fz_in[1]

    def z_update(z):
        for y in range(Y):
            value = (g2[z + 1, y + 1] - fz[z + 1, y] + fz[z, y]) / (
                1.0 - step_value * vz[z + 1, y] + step_value * vz[z, y]
            )
            out_ref[z, pl.ds(y, T, stride=Y), :] = value
    loop(0, Z, z_update)


def solution(mesh):
    n_gy, n_gz = mesh.shape["gy"], mesh.shape["gz"]

    def shards(*blocks):
        Z, Y, X = blocks[0].shape
        T = X // LANES

        def split(block):
            return block.reshape(Z, Y, T, LANES).transpose(0, 2, 1, 3).reshape(Z, T * Y, LANES)

        def rows(*lead):
            return pltpu.VMEM((*lead, T, LANES), jnp.float32)

        dma = pltpu.SemaphoreType.DMA
        padded = rows(Z + 2, Y + 2)
        plain = rows(Z, Y)
        field, dt = pl.pallas_call(
            functools.partial(kernel, n_gy, n_gz),
            out_shape=(
                jax.ShapeDtypeStruct((Z, T * Y, LANES), jnp.float32),
                jax.ShapeDtypeStruct((1, 1), jnp.float32),
            ),
            in_specs=[pl.BlockSpec(memory_space=pltpu.VMEM)] * 4,
            out_specs=(
                pl.BlockSpec(memory_space=pltpu.VMEM),
                pl.BlockSpec(memory_space=pltpu.SMEM),
            ),
            scratch_shapes=[
                padded, padded, padded, padded, padded,
                plain, plain, plain, plain,
                plain, rows(Z, Y + 1), rows(Z + 1, Y), rows(Z, Y + 1), rows(Z + 1, Y),
                rows(2, Z, 1), rows(2, 1, Y), rows(n_gy, 2), rows(n_gz, 2),
                dma((3, 8)), dma((3, 8)), dma((2,)), dma((2,)), dma((2, 2)), dma((2, 2)),
                dma((n_gy - 1,)), dma((n_gy - 1,)), dma((n_gz - 1,)), dma((n_gz - 1,)),
            ],
            compiler_params=pltpu.CompilerParams(
                collective_id=0, has_side_effects=True, vmem_limit_bytes=32 * 1024 * 1024
            ),
        )(*[split(block) for block in blocks])
        field = field.reshape(Z, T, Y, LANES).transpose(0, 2, 1, 3).reshape(Z, Y, X)
        return field, dt.reshape(())

    spec = P("gz", "gy", None)
    return jax.shard_map(
        shards, mesh=mesh, in_specs=(spec,) * 4, out_specs=(spec, P()), check_vma=False
    )
```

```python
import functools

import jax
import jax.numpy as jnp
from jax import lax
from jax.experimental import pallas as pl
from jax.experimental.pallas import tpu as pltpu
from jax.sharding import PartitionSpec as P

NEWTON = 5
LANES = 128

tilt_floor = 0.1
courant = 0.45
epsilon = 1e-06
tiny = 1e-30

MESH = pl.DeviceIdType.MESH
SIDES = [(a, b) for a in (-1, 0, 1) for b in (-1, 0, 1) if (a, b) != (0, 0)]


def lane_of(value):
    return lax.broadcasted_iota(jnp.int32, value.shape, value.ndim - 1)


def x_next(value):
    turned = pltpu.roll(value, LANES - 1, value.ndim - 1)
    carried = pltpu.roll(turned, value.shape[-2] - 1, value.ndim - 2)
    return jnp.where(lane_of(value) == LANES - 1, carried, turned)


def x_prev(value):
    turned = pltpu.roll(value, 1, value.ndim - 1)
    carried = pltpu.roll(turned, 1, value.ndim - 2)
    return jnp.where(lane_of(value) == 0, carried, turned)


def solve_offset(g, tilt_a, tilt_b, tilt_d):
    volume = jnp.clip(g, 0.0, 1.0)
    lesser = jnp.minimum(volume, 1.0 - volume)
    low = jnp.minimum(tilt_a, tilt_b)
    high = jnp.maximum(tilt_a, tilt_b)
    n1 = jnp.minimum(low, tilt_d)
    middle = jnp.maximum(low, tilt_d)
    n2 = jnp.minimum(middle, high)
    n3 = jnp.maximum(middle, high)
    summed = tilt_a + tilt_b + tilt_d
    inverse = 1.0 / jnp.maximum(n1, tiny)
    third = inverse * (1.0 / 3.0)
    product = n2 * n3
    target = 2.0 * product * lesser
    gap = jnp.maximum(n1 + n2 - n3, 0.0)
    rate = 2.0 * n2 - 0.5 * gap * (gap * inverse)
    offset = 0.5 * summed - (product - target) / rate
    for repeat in range(NEWTON - 1):
        p1 = jnp.minimum(offset, n1)
        q1 = offset - p1
        m2 = jnp.maximum(offset - n2, 0.0)
        p2 = jnp.minimum(m2, n1)
        q2 = m2 - p2
        p3 = jnp.minimum(jnp.maximum(offset - n3, 0.0), n1)
        s1, s2, s3 = p1 * p1, p2 * p2, p3 * p3
        squares = s1 - s2 - s3
        cubes = s1 * p1 - s2 * p2 - s3 * p3
        q = q1 - q2
        rate = squares * inverse + (q + q)
        volume_part = cubes * third + q * (q1 + q2 + n1)
        offset = offset - (volume_part - target) / rate
    return jnp.where(volume > 0.5, summed - offset, offset)


def face_flux(cross, offset, tilt_a, tilt_b, slope):
    turn = slope * cross
    height = jnp.abs(turn)
    reach = offset - jnp.where(turn > 0, 0.0, jnp.abs(slope) - height)

    def parts(value):
        inside = jnp.maximum(value, 0.0)
        p = jnp.minimum(inside, height)
        q = inside - p
        return p * p * p, q * (q + height)

    reach_a = reach - tilt_a
    p0, q0 = parts(reach)
    p1, q1 = parts(reach_a)
    p2, q2 = parts(reach - tilt_b)
    p3, q3 = parts(reach_a - tilt_b)
    cubes = (p0 - p1) - (p2 - p3)
    wholes = (q0 - q1) - (q2 - q3)
    combo = cubes * ((1.0 / 3.0) / jnp.maximum(height, tiny)) + wholes
    return cross * combo / (2.0 * tilt_a * tilt_b)


def kernel(
    n_gy, n_gz, f_hbm, vx_hbm, vy_hbm, vz_hbm, out_ref, dt_ref,
    f_ref, vx_ref, vy_ref, vz_ref, load_sem,
    g0, g1, g2, sx, dx, off, ta, tb, sd, vx, vy, vz, fy, fz,
    fy_in, fz_in, part_y, part_z,
    halo_send, halo_recv, vel_send, vel_recv, flux_send, flux_recv,
    py_send, py_recv, pz_send, pz_recv,
):
    Z = f_ref.shape[0]
    T = sx.shape[2]
    Y = f_ref.shape[1] // T
    loads = []
    for i, (source, target) in enumerate(
        ((f_hbm, f_ref), (vx_hbm, vx_ref), (vy_hbm, vy_ref), (vz_hbm, vz_ref))
    ):
        loads.append(pltpu.make_async_copy(source, target, load_sem.at[i]))
        loads[-1].start()
    my = lax.axis_index("gy")
    mz = lax.axis_index("gz")

    def at(dz, dy):
        return {
            "gy": lax.rem(my + dy + n_gy, n_gy),
            "gz": lax.rem(mz + dz + n_gz, n_gz),
        }

    barrier = pltpu.get_barrier_semaphore()
    greeted = [(0, i) for i in range(1, n_gy)] + [(i, 0) for i in range(1, n_gz)]
    greeted += [(a, b) for a in (-1, 1) for b in (-1, 1)]
    for dz, dy in greeted:
        pl.semaphore_signal(barrier, inc=1, device_id=at(dz, dy), device_id_type=MESH)

    def rows_of(ref, z, y):
        return ref[z, pl.ds(y, T, stride=Y), :]

    def loop(low, high, body):
        def step(i, carry):
            body(i)
            return carry
        lax.fori_loop(low, high, step, 0)

    def span(side, count):
        if side == 0:
            return pl.ds(1, count), pl.ds(1, count)
        if side > 0:
            return pl.ds(count, 1), pl.ds(0, 1)
        return pl.ds(1, 1), pl.ds(count + 1, 1)

    def halo_copies(g, which):
        copies = []
        for index, (dz, dy) in enumerate(SIDES):
            src_z, dst_z = span(dz, Z)
            src_y, dst_y = span(dy, Y)
            copies.append(pltpu.make_async_remote_copy(
                src_ref=g.at[src_z, src_y],
                dst_ref=g.at[dst_z, dst_y],
                send_sem=halo_send.at[which, index],
                recv_sem=halo_recv.at[which, index],
                device_id=at(dz, dy),
                device_id_type=MESH,
            ))
        return copies

    def fill(z, total):
        for y in range(Y):
            f = rows_of(f_ref, z, y)
            g0[z + 1, y + 1] = f
            total = total + 4.0 * f * (1.0 - f)
        return total

    loads[0].wait()
    total = lax.fori_loop(0, Z, fill, jnp.zeros((T, LANES), jnp.float32))

    def fill_velocity(z, peak):
        for y in range(Y):
            a = rows_of(vx_ref, z, y)
            b = rows_of(vy_ref, z, y)
            c = rows_of(vz_ref, z, y)
            vx[z, y] = a
            vy[z, y + 1] = b
            vz[z + 1, y] = c
            peak = jnp.maximum(peak, jnp.maximum(jnp.abs(a), jnp.maximum(jnp.abs(b), jnp.abs(c))))
        return peak

    for copy in loads[1:]:
        copy.wait()
    peak = lax.fori_loop(0, Z, fill_velocity, jnp.zeros((T, LANES), jnp.float32))
    first_row = lax.broadcasted_iota(jnp.int32, (T, LANES), 0) == 0

    def joined(sums, peaks):
        sums = jnp.broadcast_to(jnp.sum(sums, axis=0, keepdims=True), (T, LANES))
        peaks = jnp.broadcast_to(jnp.max(peaks, axis=0, keepdims=True), (T, LANES))
        return jnp.where(first_row, sums, peaks)

    def gathered(part, count):
        sums = part[0]
        peaks = part[0]
        for i in range(1, count):
            sums = sums + part[i]
            peaks = jnp.maximum(peaks, part[i])
        return jnp.where(first_row, sums, 0.0), jnp.where(first_row, 0.0, peaks)

    part_y[my] = joined(total, peak)
    pl.semaphore_wait(barrier, len(greeted))
    vel_copies = [
        pltpu.make_async_remote_copy(
            src_ref=vy.at[:, pl.ds(Y, 1)], dst_ref=vy.at[:, pl.ds(0, 1)],
            send_sem=vel_send.at[0], recv_sem=vel_recv.at[0],
            device_id=at(0, 1), device_id_type=MESH,
        ),
        pltpu.make_async_remote_copy(
            src_ref=vz.at[pl.ds(Z, 1)], dst_ref=vz.at[pl.ds(0, 1)],
            send_sem=vel_send.at[1], recv_sem=vel_recv.at[1],
            device_id=at(1, 0), device_id_type=MESH,
        ),
    ]

    def part_copies(part, mine, send, recv, count, along_y):
        copies = []
        for i in range(1, count):
            copies.append(pltpu.make_async_remote_copy(
                src_ref=part.at[mine], dst_ref=part.at[mine],
                send_sem=send.at[i - 1], recv_sem=recv.at[i - 1],
                device_id=at(0, i) if along_y else at(i, 0), device_id_type=MESH,
            ))
        return copies

    y_parts = part_copies(part_y, my, py_send, py_recv, n_gy, True)
    for copy in y_parts:
        copy.start()
    halos0 = halo_copies(g0, 0)
    for copy in halos0:
        copy.start()
    for copy in vel_copies:
        copy.start()

    def smooth_rows(g, z, y, kz, ky):
        value = g[pl.ds(z, kz), pl.ds(y, ky)]
        after, before = x_next(value), x_prev(value)
        sx[pl.ds(z, kz), pl.ds(y, ky)] = before + (value + value) + after
        dx[pl.ds(z, kz), pl.ds(y, ky)] = after - before

    def smooth_inside(g):
        loop(1, Z + 1, lambda z: smooth_rows(g, z, 1, 1, Y))

    def smooth_ghosts(g):
        smooth_rows(g, 0, 0, 1, Y + 2)
        smooth_rows(g, Z + 1, 0, 1, Y + 2)

        def edge(z):
            smooth_rows(g, z, 0, 1, 1)
            smooth_rows(g, z, Y + 1, 1, 1)
        loop(1, Z + 1, edge)

    def smooth_zero(arr):
        mid = arr[1:-1]
        return (arr[:-2] + mid) + (mid + arr[2:])

    def smooth_one(arr):
        mid = arr[:, 1:-1]
        return (arr[:, :-2] + mid) + (mid + arr[:, 2:])

    def plane(g, dim, z, y, kz, ky):
        s = sx[pl.ds(z, kz + 2), pl.ds(y, ky + 2)]
        d = dx[pl.ds(z, kz + 2), pl.ds(y, ky + 2)]
        grad_zero = smooth_one(s[2:] - s[:-2]) * (1.0 / 32.0)
        across = smooth_zero(s)
        grad_one = (across[:, 2:] - across[:, :-2]) * (1.0 / 32.0)
        grad_cells = smooth_one(smooth_zero(d)) * (1.0 / 32.0)
        slopes = (grad_zero, grad_one, grad_cells)
        slope = slopes[dim]
        tilt_a, tilt_b = [jnp.abs(slopes[e]) + tilt_floor for e in range(3) if e != dim]
        value = g[pl.ds(z + 1, kz), pl.ds(y + 1, ky)]
        where = (pl.ds(z, kz), pl.ds(y, ky))
        off[where] = solve_offset(value, tilt_a, tilt_b, jnp.abs(slope))
        ta[where] = tilt_a
        tb[where] = tilt_b
        sd[where] = slope

    half = (Y - 2) // 2
    quarter = Y // 2

    def ends(body, low, high):
        count = high - low

        def step(i):
            z = i * (Z - 1)
            body(z, low, 1, count // 2)
            body(z, low + count // 2, 1, count - count // 2)
        loop(0, 2, step)

    def sides(body, low, high):
        def step(i):
            z = low + 2 * i
            body(z, 0, 2, 1)
            body(z, Y - 1, 2, 1)
        loop(0, (high - low) // 2, step)

    def inside(body, low, high, first=1, last=None):
        count = (Y - 1 if last is None else last) - first

        def step(z):
            if count > 4:
                body(z, first, 1, count // 2)
                body(z, first + count // 2, 1, count - count // 2)
            else:
                body(z, first, 1, count)
        loop(low, high, step)

    def planes(g, dim):
        return lambda z, y, kz, ky: plane(g, dim, z, y, kz, ky)

    smooth_inside(g0)
    inside(planes(g0, 2), 1, Z // 2)
    for copy in y_parts:
        copy.wait()
    part_z[mz] = joined(*gathered(part_y, n_gy))
    z_parts = part_copies(part_z, mz, pz_send, pz_recv, n_gz, False)
    for copy in z_parts:
        copy.start()
    inside(planes(g0, 2), Z // 2, Z - 1)
    for copy in halos0:
        copy.wait()
    smooth_ghosts(g0)
    sides(planes(g0, 2), 0, Z)
    ends(planes(g0, 2), 1, Y - 1)
    for copy in z_parts:
        copy.wait()
    sums, peaks = gathered(part_z, n_gz)
    cells_all = float(Z * Y * T * LANES * n_gy * n_gz)
    share = jnp.broadcast_to(jnp.sum(sums, keepdims=True), (T, LANES)) / cells_all
    umax = jnp.broadcast_to(jnp.max(peaks, keepdims=True), (T, LANES))
    step_value = courant / ((umax + epsilon) * (1.0 + share))
    dt_ref[0, 0] = jnp.max(step_value)
    dt = step_value[None, None]

    def x_update(z, y, kz, ky):
        where = (pl.ds(z, kz), pl.ds(y, ky))
        cross = dt * vx[where]
        upward = cross > 0

        def donor(ref):
            value = ref[where]
            return jnp.where(upward, value, x_next(value))

        flux = face_flux(cross, donor(off), donor(ta), donor(tb), donor(sd))
        value = g0[pl.ds(z + 1, kz), pl.ds(y + 1, ky)]
        g1[pl.ds(z + 1, kz), pl.ds(y + 1, ky)] = (value - flux + x_prev(flux)) / (
            1.0 - cross + x_prev(cross)
        )

    sides(x_update, 0, Z)
    ends(x_update, 1, Y - 1)
    halos1 = halo_copies(g1, 1)
    for copy in halos1:
        copy.start()
    inside(x_update, 1, Z - 1)
    for copy in vel_copies:
        copy.wait()

    smooth_inside(g1)
    inside(planes(g1, 1), 1, Z - 1)
    for copy in halos1:
        copy.wait()
    smooth_ghosts(g1)
    sides(planes(g1, 1), 0, Z)

    def own_flux(velocity, where, at_face, least):
        cross = dt * velocity[at_face]
        cross = jnp.minimum(cross, 0.0) if least else jnp.maximum(cross, 0.0)
        return face_flux(cross, off[where], ta[where], tb[where], sd[where])

    def y_ends(i):
        rows = pl.ds(2 * i, 2)
        first, last = pl.ds(0, 1), pl.ds(Y - 1, 1)
        fy[rows, first] = own_flux(vy, (rows, first), (rows, first), True)
        fy[rows, pl.ds(Y, 1)] = own_flux(vy, (rows, last), (rows, pl.ds(Y, 1)), False)
    loop(0, Z // 2, y_ends)

    def flux_copies(flux, arrived, which, spans, steps):
        copies = []
        for i in range(2):
            copies.append(pltpu.make_async_remote_copy(
                src_ref=flux.at[spans[i]],
                dst_ref=arrived.at[i],
                send_sem=flux_send.at[which, i], recv_sem=flux_recv.at[which, i],
                device_id=at(*steps[i]), device_id_type=MESH,
            ))
        return copies

    every = pl.ds(0, Z)
    y_flux = flux_copies(
        fy, fy_in, 0, [(every, pl.ds(Y, 1)), (every, pl.ds(0, 1))], [(0, 1), (0, -1)]
    )
    for copy in y_flux:
        copy.start()
    ends(planes(g1, 1), 1, Y - 1)

    def between(velocity, at_face, below, above):
        cross = dt * velocity[at_face]
        upward = cross > 0

        def donor(ref):
            return jnp.where(upward, ref[below], ref[above])

        return face_flux(cross, donor(off), donor(ta), donor(tb), donor(sd))

    def y_inside(z):
        rows = pl.ds(z, 1)
        for low, count in ((1, half), (1 + half, Y - 1 - half)):
            fy[rows, pl.ds(low, count)] = between(
                vy, (rows, pl.ds(low, count)), (rows, pl.ds(low - 1, count)), (rows, pl.ds(low, count))
            )
    loop(0, Z, y_inside)

    def y_update(z, y, kz, ky):
        rows = pl.ds(z, kz)
        low, high = pl.ds(y, ky), pl.ds(y + 1, ky)
        at_cells = (pl.ds(z + 1, kz), pl.ds(y + 1, ky))
        g2[at_cells] = (g1[at_cells] - fy[rows, high] + fy[rows, low]) / (
            1.0 - dt * vy[rows, high] + dt * vy[rows, low]
        )

    inside(y_update, 0, Z)
    loop(1, Z + 1, lambda z: smooth_rows(g2, z, 2, 1, Y - 2))
    inside(planes(g2, 0), 1, Z - 1, 2, Y - 2)
    for copy in y_flux:
        copy.wait()

    def y_merge(i):
        rows = pl.ds(4 * i, 4)
        fy[rows, pl.ds(0, 1)] = fy[rows, pl.ds(0, 1)] + fy_in[0, rows]
        fy[rows, pl.ds(Y, 1)] = fy[rows, pl.ds(Y, 1)] + fy_in[1, rows]
    loop(0, Z // 4, y_merge)
    sides(y_update, 0, Z)
    halos2 = halo_copies(g2, 2)
    for copy in halos2:
        copy.start()

    def smooth_sides(z):
        smooth_rows(g2, z, 1, 1, 1)
        smooth_rows(g2, z, Y, 1, 1)
    loop(1, Z + 1, smooth_sides)

    def near_sides(i):
        z = 1 + 2 * i
        plane(g2, 0, z, 1, 2, 1)
        plane(g2, 0, z, Y - 2, 2, 1)
    loop(0, (Z - 2) // 2, near_sides)
    for copy in halos2:
        copy.wait()
    smooth_ghosts(g2)
    ends(planes(g2, 0), 0, Y)

    def z_ends(i):
        cols = pl.ds(2 * i, 2)
        first, last = pl.ds(0, 1), pl.ds(Z - 1, 1)
        fz[first, cols] = own_flux(vz, (first, cols), (first, cols), True)
        fz[pl.ds(Z, 1), cols] = own_flux(vz, (last, cols), (pl.ds(Z, 1), cols), False)
    loop(0, Y // 2, z_ends)
    z_flux = flux_copies(fz, fz_in, 1, [(pl.ds(Z, 1),), (pl.ds(0, 1),)], [(1, 0), (-1, 0)])
    for copy in z_flux:
        copy.start()
    sides(planes(g2, 0), 1, Z - 1)

    def z_inside(z):
        face, below = pl.ds(z, 1), pl.ds(z - 1, 1)
        for low, count in ((0, quarter), (quarter, Y - quarter)):
            cols = pl.ds(low, count)
            fz[face, cols] = between(vz, (face, cols), (below, cols), (face, cols))
    loop(1, Z, z_inside)
    for copy in z_flux:
        copy.wait()
    fz[pl.ds(0, 1)] = fz[pl.ds(0, 1)] + fz_in[0]
    fz[pl.ds(Z, 1)] = fz[pl.ds(Z, 1)] + fz_in[1]

    def z_update(z):
        for y in range(Y):
            value = (g2[z + 1, y + 1] - fz[z + 1, y] + fz[z, y]) / (
                1.0 - step_value * vz[z + 1, y] + step_value * vz[z, y]
            )
            out_ref[z, pl.ds(y, T, stride=Y), :] = value
    loop(0, Z, z_update)


def solution(mesh):
    n_gy, n_gz = mesh.shape["gy"], mesh.shape["gz"]

    def shards(*blocks):
        Z, Y, X = blocks[0].shape
        T = X // LANES

        def split(block):
            return block.reshape(Z, Y, T, LANES).transpose(0, 2, 1, 3).reshape(Z, T * Y, LANES)

        def rows(*lead):
            return pltpu.VMEM((*lead, T, LANES), jnp.float32)

        dma = pltpu.SemaphoreType.DMA
        padded = rows(Z + 2, Y + 2)
        plain = rows(Z, Y)
        field, dt = pl.pallas_call(
            functools.partial(kernel, n_gy, n_gz),
            out_shape=(
                jax.ShapeDtypeStruct((Z, T * Y, LANES), jnp.float32),
                jax.ShapeDtypeStruct((1, 1), jnp.float32),
            ),
            in_specs=[pl.BlockSpec(memory_space=pltpu.HBM)] * 4,
            out_specs=(
                pl.BlockSpec(memory_space=pltpu.VMEM),
                pl.BlockSpec(memory_space=pltpu.SMEM),
            ),
            scratch_shapes=[
                *[pltpu.VMEM((Z, T * Y, LANES), jnp.float32)] * 4, dma((4,)),
                padded, padded, padded, padded, padded,
                plain, plain, plain, plain,
                plain, rows(Z, Y + 1), rows(Z + 1, Y), rows(Z, Y + 1), rows(Z + 1, Y),
                rows(2, Z, 1), rows(2, 1, Y), rows(n_gy), rows(n_gz),
                dma((3, 8)), dma((3, 8)), dma((2,)), dma((2,)), dma((2, 2)), dma((2, 2)),
                dma((n_gy - 1,)), dma((n_gy - 1,)), dma((n_gz - 1,)), dma((n_gz - 1,)),
            ],
            compiler_params=pltpu.CompilerParams(
                collective_id=0, has_side_effects=True, vmem_limit_bytes=67043328
            ),
        )(*[split(block) for block in blocks])
        field = field.reshape(Z, T, Y, LANES).transpose(0, 2, 1, 3).reshape(Z, Y, X)
        return field, dt.reshape(())

    spec = P("gz", "gy", None)
    return jax.shard_map(
        shards, mesh=mesh, in_specs=(spec,) * 4, out_specs=(spec, P()), check_vma=False
    )
```

```python
import functools

import jax
import jax.numpy as jnp
from jax import lax
from jax.experimental import pallas as pl
from jax.experimental.pallas import tpu as pltpu
from jax.sharding import PartitionSpec as P

NEWTON = 5
LANES = 128
GROUP = 8

tilt_floor = 0.1
courant = 0.45
epsilon = 1e-06
tiny = 1e-30

MESH = pl.DeviceIdType.MESH
SIDES = [(a, b) for a in (-1, 0, 1) for b in (-1, 0, 1) if (a, b) != (0, 0)]


def lane_of(value):
    return lax.broadcasted_iota(jnp.int32, value.shape, value.ndim - 1)


def x_next(value):
    turned = pltpu.roll(value, LANES - 1, value.ndim - 1)
    carried = pltpu.roll(turned, value.shape[-2] - 1, value.ndim - 2)
    return jnp.where(lane_of(value) == LANES - 1, carried, turned)


def x_prev(value):
    turned = pltpu.roll(value, 1, value.ndim - 1)
    carried = pltpu.roll(turned, 1, value.ndim - 2)
    return jnp.where(lane_of(value) == 0, carried, turned)


def solve_offset(g, tilt_a, tilt_b, tilt_d):
    volume = jnp.clip(g, 0.0, 1.0)
    lesser = jnp.minimum(volume, 1.0 - volume)
    low = jnp.minimum(tilt_a, tilt_b)
    high = jnp.maximum(tilt_a, tilt_b)
    n1 = jnp.minimum(low, tilt_d)
    middle = jnp.maximum(low, tilt_d)
    n2 = jnp.minimum(middle, high)
    n3 = jnp.maximum(middle, high)
    summed = tilt_a + tilt_b + tilt_d
    inverse = 1.0 / jnp.maximum(n1, tiny)
    third = inverse * (1.0 / 3.0)
    product = n2 * n3
    target = 2.0 * product * lesser
    gap = jnp.maximum(n1 + n2 - n3, 0.0)
    rate = 2.0 * n2 - 0.5 * gap * (gap * inverse)
    offset = 0.5 * summed - (product - target) / rate
    for repeat in range(NEWTON - 1):
        p1 = jnp.minimum(offset, n1)
        q1 = offset - p1
        m2 = jnp.maximum(offset - n2, 0.0)
        p2 = jnp.minimum(m2, n1)
        q2 = m2 - p2
        p3 = jnp.minimum(jnp.maximum(offset - n3, 0.0), n1)
        s1, s2, s3 = p1 * p1, p2 * p2, p3 * p3
        squares = s1 - s2 - s3
        cubes = s1 * p1 - s2 * p2 - s3 * p3
        q = q1 - q2
        rate = squares * inverse + (q + q)
        volume_part = cubes * third + q * (q1 + q2 + n1)
        offset = offset - (volume_part - target) / rate
    return jnp.where(volume > 0.5, summed - offset, offset)


def face_flux(cross, offset, tilt_a, tilt_b, slope):
    turn = slope * cross
    height = jnp.abs(turn)
    reach = offset - jnp.where(turn > 0, 0.0, jnp.abs(slope) - height)

    def parts(value):
        inside = jnp.maximum(value, 0.0)
        p = jnp.minimum(inside, height)
        q = inside - p
        return p * p * p, q * (q + height)

    reach_a = reach - tilt_a
    p0, q0 = parts(reach)
    p1, q1 = parts(reach_a)
    p2, q2 = parts(reach - tilt_b)
    p3, q3 = parts(reach_a - tilt_b)
    cubes = (p0 - p1) - (p2 - p3)
    wholes = (q0 - q1) - (q2 - q3)
    combo = cubes * ((1.0 / 3.0) / jnp.maximum(height, tiny)) + wholes
    return cross * combo / (2.0 * tilt_a * tilt_b)


def kernel(
    n_gy, n_gz, f_hbm, vx_hbm, vy_hbm, vz_hbm, out_ref, dt_ref,
    f_ref, vx_ref, vy_ref, vz_ref, load_sem,
    g0, g1, g2, sx, dx, off, ta, tb, sd, vx, vy, vz, fy, fz,
    fy_in, fz_in, part_y, part_z,
    halo_send, halo_recv, vel_send, vel_recv, flux_send, flux_recv,
    py_send, py_recv, pz_send, pz_recv,
):
    Z = f_ref.shape[0]
    T = sx.shape[2]
    Y = f_ref.shape[1] // T
    loads = []
    for i, (source, target) in enumerate(
        ((f_hbm, f_ref), (vx_hbm, vx_ref), (vy_hbm, vy_ref), (vz_hbm, vz_ref))
    ):
        loads.append(pltpu.make_async_copy(source, target, load_sem.at[i]))
        loads[-1].start()
    my = lax.axis_index("gy")
    mz = lax.axis_index("gz")

    def at(dz, dy):
        return {
            "gy": lax.rem(my + dy + n_gy, n_gy),
            "gz": lax.rem(mz + dz + n_gz, n_gz),
        }

    barrier = pltpu.get_barrier_semaphore()
    greeted = [(0, i) for i in range(1, n_gy)] + [(i, 0) for i in range(1, n_gz)]
    greeted += [(a, b) for a in (-1, 1) for b in (-1, 1)]
    for dz, dy in greeted:
        pl.semaphore_signal(barrier, inc=1, device_id=at(dz, dy), device_id_type=MESH)

    def rows_of(ref, z, y):
        return ref[z, pl.ds(y, T, stride=Y), :]

    def gather(low, high, body, carry):
        count = high - low
        grouped = max(u for u in range(1, GROUP + 1) if count % u == 0)

        def step(i, carry):
            for u in range(grouped):
                carry = body(low + i * grouped + u, carry)
            return carry
        return lax.fori_loop(0, count // grouped, step, carry)

    def loop(low, high, body):
        def step(i, carry):
            body(i)
            return carry
        gather(low, high, step, 0)

    def span(side, count):
        if side == 0:
            return pl.ds(1, count), pl.ds(1, count)
        if side > 0:
            return pl.ds(count, 1), pl.ds(0, 1)
        return pl.ds(1, 1), pl.ds(count + 1, 1)

    def halo_copies(g, which):
        copies = []
        for index, (dz, dy) in enumerate(SIDES):
            src_z, dst_z = span(dz, Z)
            src_y, dst_y = span(dy, Y)
            copies.append(pltpu.make_async_remote_copy(
                src_ref=g.at[src_z, src_y],
                dst_ref=g.at[dst_z, dst_y],
                send_sem=halo_send.at[which, index],
                recv_sem=halo_recv.at[which, index],
                device_id=at(dz, dy),
                device_id_type=MESH,
            ))
        return copies

    def fill(z, total):
        for y in range(Y):
            f = rows_of(f_ref, z, y)
            g0[z + 1, y + 1] = f
            total = total + 4.0 * f * (1.0 - f)
        return total

    loads[0].wait()
    total = gather(0, Z, fill, jnp.zeros((T, LANES), jnp.float32))

    def fill_velocity(z, peak):
        for y in range(Y):
            a = rows_of(vx_ref, z, y)
            b = rows_of(vy_ref, z, y)
            c = rows_of(vz_ref, z, y)
            vx[z, y] = a
            vy[z, y + 1] = b
            vz[z + 1, y] = c
            peak = jnp.maximum(peak, jnp.maximum(jnp.abs(a), jnp.maximum(jnp.abs(b), jnp.abs(c))))
        return peak

    for copy in loads[1:]:
        copy.wait()
    peak = gather(0, Z, fill_velocity, jnp.zeros((T, LANES), jnp.float32))
    first_row = lax.broadcasted_iota(jnp.int32, (T, LANES), 0) == 0

    def joined(sums, peaks):
        sums = jnp.broadcast_to(jnp.sum(sums, axis=0, keepdims=True), (T, LANES))
        peaks = jnp.broadcast_to(jnp.max(peaks, axis=0, keepdims=True), (T, LANES))
        return jnp.where(first_row, sums, peaks)

    def gathered(part, count):
        sums = part[0]
        peaks = part[0]
        for i in range(1, count):
            sums = sums + part[i]
            peaks = jnp.maximum(peaks, part[i])
        return jnp.where(first_row, sums, 0.0), jnp.where(first_row, 0.0, peaks)

    part_y[my] = joined(total, peak)
    pl.semaphore_wait(barrier, len(greeted))
    vel_copies = [
        pltpu.make_async_remote_copy(
            src_ref=vy.at[:, pl.ds(Y, 1)], dst_ref=vy.at[:, pl.ds(0, 1)],
            send_sem=vel_send.at[0], recv_sem=vel_recv.at[0],
            device_id=at(0, 1), device_id_type=MESH,
        ),
        pltpu.make_async_remote_copy(
            src_ref=vz.at[pl.ds(Z, 1)], dst_ref=vz.at[pl.ds(0, 1)],
            send_sem=vel_send.at[1], recv_sem=vel_recv.at[1],
            device_id=at(1, 0), device_id_type=MESH,
        ),
    ]

    def part_copies(part, mine, send, recv, count, along_y):
        copies = []
        for i in range(1, count):
            copies.append(pltpu.make_async_remote_copy(
                src_ref=part.at[mine], dst_ref=part.at[mine],
                send_sem=send.at[i - 1], recv_sem=recv.at[i - 1],
                device_id=at(0, i) if along_y else at(i, 0), device_id_type=MESH,
            ))
        return copies

    y_parts = part_copies(part_y, my, py_send, py_recv, n_gy, True)
    for copy in y_parts:
        copy.start()
    halos0 = halo_copies(g0, 0)
    for copy in halos0:
        copy.start()
    for copy in vel_copies:
        copy.start()

    def smooth_rows(g, z, y, kz, ky):
        value = g[pl.ds(z, kz), pl.ds(y, ky)]
        after, before = x_next(value), x_prev(value)
        sx[pl.ds(z, kz), pl.ds(y, ky)] = before + (value + value) + after
        dx[pl.ds(z, kz), pl.ds(y, ky)] = after - before

    def smooth_inside(g):
        loop(1, Z + 1, lambda z: smooth_rows(g, z, 1, 1, Y))

    def smooth_ghosts(g):
        smooth_rows(g, 0, 0, 1, Y + 2)
        smooth_rows(g, Z + 1, 0, 1, Y + 2)

        def edge(z):
            smooth_rows(g, z, 0, 1, 1)
            smooth_rows(g, z, Y + 1, 1, 1)
        loop(1, Z + 1, edge)

    def smooth_zero(arr):
        mid = arr[1:-1]
        return (arr[:-2] + mid) + (mid + arr[2:])

    def smooth_one(arr):
        mid = arr[:, 1:-1]
        return (arr[:, :-2] + mid) + (mid + arr[:, 2:])

    def plane(g, dim, z, y, kz, ky):
        s = sx[pl.ds(z, kz + 2), pl.ds(y, ky + 2)]
        d = dx[pl.ds(z, kz + 2), pl.ds(y, ky + 2)]
        grad_zero = smooth_one(s[2:] - s[:-2]) * (1.0 / 32.0)
        across = smooth_zero(s)
        grad_one = (across[:, 2:] - across[:, :-2]) * (1.0 / 32.0)
        grad_cells = smooth_one(smooth_zero(d)) * (1.0 / 32.0)
        slopes = (grad_zero, grad_one, grad_cells)
        slope = slopes[dim]
        tilt_a, tilt_b = [jnp.abs(slopes[e]) + tilt_floor for e in range(3) if e != dim]
        value = g[pl.ds(z + 1, kz), pl.ds(y + 1, ky)]
        where = (pl.ds(z, kz), pl.ds(y, ky))
        off[where] = solve_offset(value, tilt_a, tilt_b, jnp.abs(slope))
        ta[where] = tilt_a
        tb[where] = tilt_b
        sd[where] = slope

    half = (Y - 2) // 2
    quarter = Y // 2

    def ends(body, low, high):
        count = high - low

        def step(i):
            z = i * (Z - 1)
            body(z, low, 1, count // 2)
            body(z, low + count // 2, 1, count - count // 2)
        loop(0, 2, step)

    def sides(body, low, high):
        def step(i):
            z = low + 2 * i
            body(z, 0, 2, 1)
            body(z, Y - 1, 2, 1)
        loop(0, (high - low) // 2, step)

    def inside(body, low, high, first=1, last=None):
        count = (Y - 1 if last is None else last) - first

        def step(z):
            if count > 4:
                body(z, first, 1, count // 2)
                body(z, first + count // 2, 1, count - count // 2)
            else:
                body(z, first, 1, count)
        loop(low, high, step)

    def planes(g, dim):
        return lambda z, y, kz, ky: plane(g, dim, z, y, kz, ky)

    smooth_inside(g0)
    inside(planes(g0, 2), 1, Z // 2)
    for copy in y_parts:
        copy.wait()
    part_z[mz] = joined(*gathered(part_y, n_gy))
    z_parts = part_copies(part_z, mz, pz_send, pz_recv, n_gz, False)
    for copy in z_parts:
        copy.start()
    inside(planes(g0, 2), Z // 2, Z - 1)
    for copy in halos0:
        copy.wait()
    smooth_ghosts(g0)
    sides(planes(g0, 2), 0, Z)
    ends(planes(g0, 2), 1, Y - 1)
    for copy in z_parts:
        copy.wait()
    sums, peaks = gathered(part_z, n_gz)
    cells_all = float(Z * Y * T * LANES * n_gy * n_gz)
    share = jnp.broadcast_to(jnp.sum(sums, keepdims=True), (T, LANES)) / cells_all
    umax = jnp.broadcast_to(jnp.max(peaks, keepdims=True), (T, LANES))
    step_value = courant / ((umax + epsilon) * (1.0 + share))
    dt_ref[0, 0] = jnp.max(step_value)
    dt = step_value[None, None]

    def x_update(z, y, kz, ky):
        where = (pl.ds(z, kz), pl.ds(y, ky))
        cross = dt * vx[where]
        upward = cross > 0

        def donor(ref):
            value = ref[where]
            return jnp.where(upward, value, x_next(value))

        flux = face_flux(cross, donor(off), donor(ta), donor(tb), donor(sd))
        value = g0[pl.ds(z + 1, kz), pl.ds(y + 1, ky)]
        g1[pl.ds(z + 1, kz), pl.ds(y + 1, ky)] = (value - flux + x_prev(flux)) / (
            1.0 - cross + x_prev(cross)
        )

    sides(x_update, 0, Z)
    ends(x_update, 1, Y - 1)
    halos1 = halo_copies(g1, 1)
    for copy in halos1:
        copy.start()
    inside(x_update, 1, Z - 1)
    for copy in vel_copies:
        copy.wait()

    smooth_inside(g1)
    inside(planes(g1, 1), 1, Z - 1)
    for copy in halos1:
        copy.wait()
    smooth_ghosts(g1)
    sides(planes(g1, 1), 0, Z)

    def own_flux(velocity, where, at_face, least):
        cross = dt * velocity[at_face]
        cross = jnp.minimum(cross, 0.0) if least else jnp.maximum(cross, 0.0)
        return face_flux(cross, off[where], ta[where], tb[where], sd[where])

    def y_ends(i):
        rows = pl.ds(2 * i, 2)
        first, last = pl.ds(0, 1), pl.ds(Y - 1, 1)
        fy[rows, first] = own_flux(vy, (rows, first), (rows, first), True)
        fy[rows, pl.ds(Y, 1)] = own_flux(vy, (rows, last), (rows, pl.ds(Y, 1)), False)
    loop(0, Z // 2, y_ends)

    def flux_copies(flux, arrived, which, spans, steps):
        copies = []
        for i in range(2):
            copies.append(pltpu.make_async_remote_copy(
                src_ref=flux.at[spans[i]],
                dst_ref=arrived.at[i],
                send_sem=flux_send.at[which, i], recv_sem=flux_recv.at[which, i],
                device_id=at(*steps[i]), device_id_type=MESH,
            ))
        return copies

    every = pl.ds(0, Z)
    y_flux = flux_copies(
        fy, fy_in, 0, [(every, pl.ds(Y, 1)), (every, pl.ds(0, 1))], [(0, 1), (0, -1)]
    )
    for copy in y_flux:
        copy.start()
    ends(planes(g1, 1), 1, Y - 1)

    def between(velocity, at_face, below, above):
        cross = dt * velocity[at_face]
        upward = cross > 0

        def donor(ref):
            return jnp.where(upward, ref[below], ref[above])

        return face_flux(cross, donor(off), donor(ta), donor(tb), donor(sd))

    def y_inside(z):
        rows = pl.ds(z, 1)
        for low, count in ((1, half), (1 + half, Y - 1 - half)):
            fy[rows, pl.ds(low, count)] = between(
                vy, (rows, pl.ds(low, count)), (rows, pl.ds(low - 1, count)), (rows, pl.ds(low, count))
            )
    loop(0, Z, y_inside)

    def y_update(z, y, kz, ky):
        rows = pl.ds(z, kz)
        low, high = pl.ds(y, ky), pl.ds(y + 1, ky)
        at_cells = (pl.ds(z + 1, kz), pl.ds(y + 1, ky))
        g2[at_cells] = (g1[at_cells] - fy[rows, high] + fy[rows, low]) / (
            1.0 - dt * vy[rows, high] + dt * vy[rows, low]
        )

    inside(y_update, 0, Z)
    loop(1, Z + 1, lambda z: smooth_rows(g2, z, 2, 1, Y - 2))
    inside(planes(g2, 0), 1, Z - 1, 2, Y - 2)
    for copy in y_flux:
        copy.wait()

    def y_merge(i):
        rows = pl.ds(4 * i, 4)
        fy[rows, pl.ds(0, 1)] = fy[rows, pl.ds(0, 1)] + fy_in[0, rows]
        fy[rows, pl.ds(Y, 1)] = fy[rows, pl.ds(Y, 1)] + fy_in[1, rows]
    loop(0, Z // 4, y_merge)
    sides(y_update, 0, Z)
    halos2 = halo_copies(g2, 2)
    for copy in halos2:
        copy.start()

    def smooth_sides(z):
        smooth_rows(g2, z, 1, 1, 1)
        smooth_rows(g2, z, Y, 1, 1)
    loop(1, Z + 1, smooth_sides)

    def near_sides(i):
        z = 1 + 2 * i
        plane(g2, 0, z, 1, 2, 1)
        plane(g2, 0, z, Y - 2, 2, 1)
    loop(0, (Z - 2) // 2, near_sides)
    for copy in halos2:
        copy.wait()
    smooth_ghosts(g2)
    ends(planes(g2, 0), 0, Y)

    def z_ends(i):
        cols = pl.ds(2 * i, 2)
        first, last = pl.ds(0, 1), pl.ds(Z - 1, 1)
        fz[first, cols] = own_flux(vz, (first, cols), (first, cols), True)
        fz[pl.ds(Z, 1), cols] = own_flux(vz, (last, cols), (pl.ds(Z, 1), cols), False)
    loop(0, Y // 2, z_ends)
    z_flux = flux_copies(fz, fz_in, 1, [(pl.ds(Z, 1),), (pl.ds(0, 1),)], [(1, 0), (-1, 0)])
    for copy in z_flux:
        copy.start()
    sides(planes(g2, 0), 1, Z - 1)

    def z_inside(z):
        face, below = pl.ds(z, 1), pl.ds(z - 1, 1)
        for low, count in ((0, quarter), (quarter, Y - quarter)):
            cols = pl.ds(low, count)
            fz[face, cols] = between(vz, (face, cols), (below, cols), (face, cols))
    loop(1, Z, z_inside)
    for copy in z_flux:
        copy.wait()
    fz[pl.ds(0, 1)] = fz[pl.ds(0, 1)] + fz_in[0]
    fz[pl.ds(Z, 1)] = fz[pl.ds(Z, 1)] + fz_in[1]

    def z_update(z):
        for y in range(Y):
            value = (g2[z + 1, y + 1] - fz[z + 1, y] + fz[z, y]) / (
                1.0 - step_value * vz[z + 1, y] + step_value * vz[z, y]
            )
            out_ref[z, pl.ds(y, T, stride=Y), :] = value
    loop(0, Z, z_update)


def solution(mesh):
    n_gy, n_gz = mesh.shape["gy"], mesh.shape["gz"]

    def shards(*blocks):
        Z, Y, X = blocks[0].shape
        T = X // LANES

        def split(block):
            return block.reshape(Z, Y, T, LANES).transpose(0, 2, 1, 3).reshape(Z, T * Y, LANES)

        def rows(*lead):
            return pltpu.VMEM((*lead, T, LANES), jnp.float32)

        dma = pltpu.SemaphoreType.DMA
        padded = rows(Z + 2, Y + 2)
        plain = rows(Z, Y)
        field, dt = pl.pallas_call(
            functools.partial(kernel, n_gy, n_gz),
            out_shape=(
                jax.ShapeDtypeStruct((Z, T * Y, LANES), jnp.float32),
                jax.ShapeDtypeStruct((1, 1), jnp.float32),
            ),
            in_specs=[pl.BlockSpec(memory_space=pltpu.HBM)] * 4,
            out_specs=(
                pl.BlockSpec(memory_space=pltpu.VMEM),
                pl.BlockSpec(memory_space=pltpu.SMEM),
            ),
            scratch_shapes=[
                *[pltpu.VMEM((Z, T * Y, LANES), jnp.float32)] * 4, dma((4,)),
                padded, padded, padded, padded, padded,
                plain, plain, plain, plain,
                plain, rows(Z, Y + 1), rows(Z + 1, Y), rows(Z, Y + 1), rows(Z + 1, Y),
                rows(2, Z, 1), rows(2, 1, Y), rows(n_gy), rows(n_gz),
                dma((3, 8)), dma((3, 8)), dma((2,)), dma((2,)), dma((2, 2)), dma((2, 2)),
                dma((n_gy - 1,)), dma((n_gy - 1,)), dma((n_gz - 1,)), dma((n_gz - 1,)),
            ],
            compiler_params=pltpu.CompilerParams(
                collective_id=0, has_side_effects=True, vmem_limit_bytes=67043328
            ),
        )(*[split(block) for block in blocks])
        field = field.reshape(Z, T, Y, LANES).transpose(0, 2, 1, 3).reshape(Z, Y, X)
        return field, dt.reshape(())

    spec = P("gz", "gy", None)
    return jax.shard_map(
        shards, mesh=mesh, in_specs=(spec,) * 4, out_specs=(spec, P()), check_vma=False
    )
```

```python
import functools

import jax
import jax.numpy as jnp
from jax import lax
from jax.experimental import pallas as pl
from jax.experimental.pallas import tpu as pltpu
from jax.sharding import PartitionSpec as P

NEWTON = 5
LANES = 128
GROUP = 16

tilt_floor = 0.1
courant = 0.45
epsilon = 1e-06
tiny = 1e-30

MESH = pl.DeviceIdType.MESH
SIDES = [(a, b) for a in (-1, 0, 1) for b in (-1, 0, 1) if (a, b) != (0, 0)]


def lane_of(value):
    return lax.broadcasted_iota(jnp.int32, value.shape, value.ndim - 1)


def x_next(value):
    turned = pltpu.roll(value, LANES - 1, value.ndim - 1)
    carried = pltpu.roll(turned, value.shape[-2] - 1, value.ndim - 2)
    return jnp.where(lane_of(value) == LANES - 1, carried, turned)


def x_prev(value):
    turned = pltpu.roll(value, 1, value.ndim - 1)
    carried = pltpu.roll(turned, 1, value.ndim - 2)
    return jnp.where(lane_of(value) == 0, carried, turned)


def solve_offset(g, tilt_a, tilt_b, tilt_d):
    volume = jnp.clip(g, 0.0, 1.0)
    lesser = jnp.minimum(volume, 1.0 - volume)
    low = jnp.minimum(tilt_a, tilt_b)
    high = jnp.maximum(tilt_a, tilt_b)
    n1 = jnp.minimum(low, tilt_d)
    middle = jnp.maximum(low, tilt_d)
    n2 = jnp.minimum(middle, high)
    n3 = jnp.maximum(middle, high)
    summed = tilt_a + tilt_b + tilt_d
    inverse = 1.0 / jnp.maximum(n1, tiny)
    third = inverse * (1.0 / 3.0)
    product = n2 * n3
    target = 2.0 * product * lesser
    gap = jnp.maximum(n1 + n2 - n3, 0.0)
    rate = 2.0 * n2 - 0.5 * gap * (gap * inverse)
    offset = 0.5 * summed - (product - target) / rate
    for repeat in range(NEWTON - 1):
        p1 = jnp.minimum(offset, n1)
        q1 = offset - p1
        m2 = jnp.maximum(offset - n2, 0.0)
        p2 = jnp.minimum(m2, n1)
        q2 = m2 - p2
        p3 = jnp.minimum(jnp.maximum(offset - n3, 0.0), n1)
        s1, s2, s3 = p1 * p1, p2 * p2, p3 * p3
        squares = s1 - s2 - s3
        cubes = s1 * p1 - s2 * p2 - s3 * p3
        q = q1 - q2
        rate = squares * inverse + (q + q)
        volume_part = cubes * third + q * (q1 + q2 + n1)
        offset = offset - (volume_part - target) / rate
    return jnp.where(volume > 0.5, summed - offset, offset)


def face_flux(cross, offset, tilt_a, tilt_b, slope):
    turn = slope * cross
    height = jnp.abs(turn)
    reach = offset - jnp.where(turn > 0, 0.0, jnp.abs(slope) - height)

    def parts(value):
        inside = jnp.maximum(value, 0.0)
        p = jnp.minimum(inside, height)
        q = inside - p
        return p * p * p, q * (q + height)

    reach_a = reach - tilt_a
    p0, q0 = parts(reach)
    p1, q1 = parts(reach_a)
    p2, q2 = parts(reach - tilt_b)
    p3, q3 = parts(reach_a - tilt_b)
    cubes = (p0 - p1) - (p2 - p3)
    wholes = (q0 - q1) - (q2 - q3)
    combo = cubes * ((1.0 / 3.0) / jnp.maximum(height, tiny)) + wholes
    return cross * combo / (2.0 * tilt_a * tilt_b)


def kernel(
    n_gy, n_gz, f_hbm, vx_hbm, vy_hbm, vz_hbm, out_ref, dt_ref,
    f_ref, vx_ref, vy_ref, vz_ref, load_sem,
    g0, g1, g2, sx, dx, off, ta, tb, sd, vx, vy, vz, fy, fz,
    fy_in, fz_in, part_y, part_z,
    halo_send, halo_recv, vel_send, vel_recv, flux_send, flux_recv,
    py_send, py_recv, pz_send, pz_recv,
):
    Z = f_ref.shape[0]
    T = sx.shape[2]
    Y = f_ref.shape[1] // T
    loads = []
    for i, (source, target) in enumerate(
        ((f_hbm, f_ref), (vx_hbm, vx_ref), (vy_hbm, vy_ref), (vz_hbm, vz_ref))
    ):
        loads.append(pltpu.make_async_copy(source, target, load_sem.at[i]))
        loads[-1].start()
    my = lax.axis_index("gy")
    mz = lax.axis_index("gz")

    def at(dz, dy):
        return {
            "gy": lax.rem(my + dy + n_gy, n_gy),
            "gz": lax.rem(mz + dz + n_gz, n_gz),
        }

    barrier = pltpu.get_barrier_semaphore()
    greeted = [(0, i) for i in range(1, n_gy)] + [(i, 0) for i in range(1, n_gz)]
    greeted += [(a, b) for a in (-1, 1) for b in (-1, 1)]
    for dz, dy in greeted:
        pl.semaphore_signal(barrier, inc=1, device_id=at(dz, dy), device_id_type=MESH)

    def rows_of(ref, z, y):
        return ref[z, pl.ds(y, T, stride=Y), :]

    def gather(low, high, body, carry):
        count = high - low
        grouped = max(u for u in range(1, GROUP + 1) if count % u == 0)

        def step(i, carry):
            for u in range(grouped):
                carry = body(low + i * grouped + u, carry)
            return carry
        return lax.fori_loop(0, count // grouped, step, carry)

    def loop(low, high, body):
        def step(i, carry):
            body(i)
            return carry
        gather(low, high, step, 0)

    def span(side, count):
        if side == 0:
            return pl.ds(1, count), pl.ds(1, count)
        if side > 0:
            return pl.ds(count, 1), pl.ds(0, 1)
        return pl.ds(1, 1), pl.ds(count + 1, 1)

    def halo_copies(g, which):
        copies = []
        for index, (dz, dy) in enumerate(SIDES):
            src_z, dst_z = span(dz, Z)
            src_y, dst_y = span(dy, Y)
            copies.append(pltpu.make_async_remote_copy(
                src_ref=g.at[src_z, src_y],
                dst_ref=g.at[dst_z, dst_y],
                send_sem=halo_send.at[which, index],
                recv_sem=halo_recv.at[which, index],
                device_id=at(dz, dy),
                device_id_type=MESH,
            ))
        return copies

    def fill(z, total):
        for y in range(Y):
            f = rows_of(f_ref, z, y)
            g0[z + 1, y + 1] = f
            total = total + 4.0 * f * (1.0 - f)
        return total

    loads[0].wait()
    total = gather(0, Z, fill, jnp.zeros((T, LANES), jnp.float32))

    def fill_velocity(z, peak):
        for y in range(Y):
            a = rows_of(vx_ref, z, y)
            b = rows_of(vy_ref, z, y)
            c = rows_of(vz_ref, z, y)
            vx[z, y] = a
            vy[z, y + 1] = b
            vz[z + 1, y] = c
            peak = jnp.maximum(peak, jnp.maximum(jnp.abs(a), jnp.maximum(jnp.abs(b), jnp.abs(c))))
        return peak

    for copy in loads[1:]:
        copy.wait()
    peak = gather(0, Z, fill_velocity, jnp.zeros((T, LANES), jnp.float32))
    first_row = lax.broadcasted_iota(jnp.int32, (T, LANES), 0) == 0

    def joined(sums, peaks):
        sums = jnp.broadcast_to(jnp.sum(sums, axis=0, keepdims=True), (T, LANES))
        peaks = jnp.broadcast_to(jnp.max(peaks, axis=0, keepdims=True), (T, LANES))
        return jnp.where(first_row, sums, peaks)

    def gathered(part, count):
        sums = part[0]
        peaks = part[0]
        for i in range(1, count):
            sums = sums + part[i]
            peaks = jnp.maximum(peaks, part[i])
        return jnp.where(first_row, sums, 0.0), jnp.where(first_row, 0.0, peaks)

    part_y[my] = joined(total, peak)
    pl.semaphore_wait(barrier, len(greeted))
    vel_copies = [
        pltpu.make_async_remote_copy(
            src_ref=vy.at[:, pl.ds(Y, 1)], dst_ref=vy.at[:, pl.ds(0, 1)],
            send_sem=vel_send.at[0], recv_sem=vel_recv.at[0],
            device_id=at(0, 1), device_id_type=MESH,
        ),
        pltpu.make_async_remote_copy(
            src_ref=vz.at[pl.ds(Z, 1)], dst_ref=vz.at[pl.ds(0, 1)],
            send_sem=vel_send.at[1], recv_sem=vel_recv.at[1],
            device_id=at(1, 0), device_id_type=MESH,
        ),
    ]

    def part_copies(part, mine, send, recv, count, along_y):
        copies = []
        for i in range(1, count):
            copies.append(pltpu.make_async_remote_copy(
                src_ref=part.at[mine], dst_ref=part.at[mine],
                send_sem=send.at[i - 1], recv_sem=recv.at[i - 1],
                device_id=at(0, i) if along_y else at(i, 0), device_id_type=MESH,
            ))
        return copies

    y_parts = part_copies(part_y, my, py_send, py_recv, n_gy, True)
    for copy in y_parts:
        copy.start()
    halos0 = halo_copies(g0, 0)
    for copy in halos0:
        copy.start()
    for copy in vel_copies:
        copy.start()

    def smooth_rows(g, z, y, kz, ky):
        value = g[pl.ds(z, kz), pl.ds(y, ky)]
        after, before = x_next(value), x_prev(value)
        sx[pl.ds(z, kz), pl.ds(y, ky)] = before + (value + value) + after
        dx[pl.ds(z, kz), pl.ds(y, ky)] = after - before

    def smooth_inside(g):
        loop(1, Z + 1, lambda z: smooth_rows(g, z, 1, 1, Y))

    def smooth_ghosts(g):
        smooth_rows(g, 0, 0, 1, Y + 2)
        smooth_rows(g, Z + 1, 0, 1, Y + 2)

        def edge(z):
            smooth_rows(g, z, 0, 1, 1)
            smooth_rows(g, z, Y + 1, 1, 1)
        loop(1, Z + 1, edge)

    def smooth_zero(arr):
        mid = arr[1:-1]
        return (arr[:-2] + mid) + (mid + arr[2:])

    def smooth_one(arr):
        mid = arr[:, 1:-1]
        return (arr[:, :-2] + mid) + (mid + arr[:, 2:])

    def plane(g, dim, z, y, kz, ky):
        s = sx[pl.ds(z, kz + 2), pl.ds(y, ky + 2)]
        d = dx[pl.ds(z, kz + 2), pl.ds(y, ky + 2)]
        grad_zero = smooth_one(s[2:] - s[:-2]) * (1.0 / 32.0)
        across = smooth_zero(s)
        grad_one = (across[:, 2:] - across[:, :-2]) * (1.0 / 32.0)
        grad_cells = smooth_one(smooth_zero(d)) * (1.0 / 32.0)
        slopes = (grad_zero, grad_one, grad_cells)
        slope = slopes[dim]
        tilt_a, tilt_b = [jnp.abs(slopes[e]) + tilt_floor for e in range(3) if e != dim]
        value = g[pl.ds(z + 1, kz), pl.ds(y + 1, ky)]
        where = (pl.ds(z, kz), pl.ds(y, ky))
        off[where] = solve_offset(value, tilt_a, tilt_b, jnp.abs(slope))
        ta[where] = tilt_a
        tb[where] = tilt_b
        sd[where] = slope

    half = (Y - 2) // 2
    quarter = Y // 2

    def ends(body, low, high):
        count = high - low

        def step(i):
            z = i * (Z - 1)
            body(z, low, 1, count // 2)
            body(z, low + count // 2, 1, count - count // 2)
        loop(0, 2, step)

    def sides(body, low, high):
        def step(i):
            z = low + 2 * i
            body(z, 0, 2, 1)
            body(z, Y - 1, 2, 1)
        loop(0, (high - low) // 2, step)

    def inside(body, low, high, first=1, last=None):
        count = (Y - 1 if last is None else last) - first

        def step(z):
            if count > 4:
                body(z, first, 1, count // 2)
                body(z, first + count // 2, 1, count - count // 2)
            else:
                body(z, first, 1, count)
        loop(low, high, step)

    def planes(g, dim):
        return lambda z, y, kz, ky: plane(g, dim, z, y, kz, ky)

    smooth_inside(g0)
    inside(planes(g0, 2), 1, Z // 2)
    for copy in y_parts:
        copy.wait()
    part_z[mz] = joined(*gathered(part_y, n_gy))
    z_parts = part_copies(part_z, mz, pz_send, pz_recv, n_gz, False)
    for copy in z_parts:
        copy.start()
    inside(planes(g0, 2), Z // 2, Z - 1)
    for copy in halos0:
        copy.wait()
    smooth_ghosts(g0)
    sides(planes(g0, 2), 0, Z)
    ends(planes(g0, 2), 1, Y - 1)
    for copy in z_parts:
        copy.wait()
    sums, peaks = gathered(part_z, n_gz)
    cells_all = float(Z * Y * T * LANES * n_gy * n_gz)
    share = jnp.broadcast_to(jnp.sum(sums, keepdims=True), (T, LANES)) / cells_all
    umax = jnp.broadcast_to(jnp.max(peaks, keepdims=True), (T, LANES))
    step_value = courant / ((umax + epsilon) * (1.0 + share))
    dt_ref[0, 0] = jnp.max(step_value)
    dt = step_value[None, None]

    def x_update(z, y, kz, ky):
        where = (pl.ds(z, kz), pl.ds(y, ky))
        cross = dt * vx[where]
        upward = cross > 0

        def donor(ref):
            value = ref[where]
            return jnp.where(upward, value, x_next(value))

        flux = face_flux(cross, donor(off), donor(ta), donor(tb), donor(sd))
        value = g0[pl.ds(z + 1, kz), pl.ds(y + 1, ky)]
        g1[pl.ds(z + 1, kz), pl.ds(y + 1, ky)] = (value - flux + x_prev(flux)) / (
            1.0 - cross + x_prev(cross)
        )

    sides(x_update, 0, Z)
    ends(x_update, 1, Y - 1)
    halos1 = halo_copies(g1, 1)
    for copy in halos1:
        copy.start()
    inside(x_update, 1, Z - 1)
    for copy in vel_copies:
        copy.wait()

    smooth_inside(g1)
    inside(planes(g1, 1), 1, Z - 1)
    for copy in halos1:
        copy.wait()
    smooth_ghosts(g1)
    sides(planes(g1, 1), 0, Z)

    def own_flux(velocity, where, at_face, least):
        cross = dt * velocity[at_face]
        cross = jnp.minimum(cross, 0.0) if least else jnp.maximum(cross, 0.0)
        return face_flux(cross, off[where], ta[where], tb[where], sd[where])

    def y_ends(i):
        rows = pl.ds(2 * i, 2)
        first, last = pl.ds(0, 1), pl.ds(Y - 1, 1)
        fy[rows, first] = own_flux(vy, (rows, first), (rows, first), True)
        fy[rows, pl.ds(Y, 1)] = own_flux(vy, (rows, last), (rows, pl.ds(Y, 1)), False)
    loop(0, Z // 2, y_ends)

    def flux_copies(flux, arrived, which, spans, steps):
        copies = []
        for i in range(2):
            copies.append(pltpu.make_async_remote_copy(
                src_ref=flux.at[spans[i]],
                dst_ref=arrived.at[i],
                send_sem=flux_send.at[which, i], recv_sem=flux_recv.at[which, i],
                device_id=at(*steps[i]), device_id_type=MESH,
            ))
        return copies

    every = pl.ds(0, Z)
    y_flux = flux_copies(
        fy, fy_in, 0, [(every, pl.ds(Y, 1)), (every, pl.ds(0, 1))], [(0, 1), (0, -1)]
    )
    for copy in y_flux:
        copy.start()
    ends(planes(g1, 1), 1, Y - 1)

    def between(velocity, at_face, below, above):
        cross = dt * velocity[at_face]
        upward = cross > 0

        def donor(ref):
            return jnp.where(upward, ref[below], ref[above])

        return face_flux(cross, donor(off), donor(ta), donor(tb), donor(sd))

    def y_inside(z):
        rows = pl.ds(z, 1)
        for low, count in ((1, half), (1 + half, Y - 1 - half)):
            fy[rows, pl.ds(low, count)] = between(
                vy, (rows, pl.ds(low, count)), (rows, pl.ds(low - 1, count)), (rows, pl.ds(low, count))
            )
    loop(0, Z, y_inside)

    def y_update(z, y, kz, ky):
        rows = pl.ds(z, kz)
        low, high = pl.ds(y, ky), pl.ds(y + 1, ky)
        at_cells = (pl.ds(z + 1, kz), pl.ds(y + 1, ky))
        g2[at_cells] = (g1[at_cells] - fy[rows, high] + fy[rows, low]) / (
            1.0 - dt * vy[rows, high] + dt * vy[rows, low]
        )

    inside(y_update, 0, Z)
    loop(1, Z + 1, lambda z: smooth_rows(g2, z, 2, 1, Y - 2))
    inside(planes(g2, 0), 1, Z - 1, 2, Y - 2)
    for copy in y_flux:
        copy.wait()

    def y_merge(i):
        rows = pl.ds(4 * i, 4)
        fy[rows, pl.ds(0, 1)] = fy[rows, pl.ds(0, 1)] + fy_in[0, rows]
        fy[rows, pl.ds(Y, 1)] = fy[rows, pl.ds(Y, 1)] + fy_in[1, rows]
    loop(0, Z // 4, y_merge)
    sides(y_update, 0, Z)
    halos2 = halo_copies(g2, 2)
    for copy in halos2:
        copy.start()

    def smooth_sides(z):
        smooth_rows(g2, z, 1, 1, 1)
        smooth_rows(g2, z, Y, 1, 1)
    loop(1, Z + 1, smooth_sides)

    def near_sides(i):
        z = 1 + 2 * i
        plane(g2, 0, z, 1, 2, 1)
        plane(g2, 0, z, Y - 2, 2, 1)
    loop(0, (Z - 2) // 2, near_sides)
    for copy in halos2:
        copy.wait()
    smooth_ghosts(g2)
    ends(planes(g2, 0), 0, Y)

    def z_ends(i):
        cols = pl.ds(2 * i, 2)
        first, last = pl.ds(0, 1), pl.ds(Z - 1, 1)
        fz[first, cols] = own_flux(vz, (first, cols), (first, cols), True)
        fz[pl.ds(Z, 1), cols] = own_flux(vz, (last, cols), (pl.ds(Z, 1), cols), False)
    loop(0, Y // 2, z_ends)
    z_flux = flux_copies(fz, fz_in, 1, [(pl.ds(Z, 1),), (pl.ds(0, 1),)], [(1, 0), (-1, 0)])
    for copy in z_flux:
        copy.start()
    sides(planes(g2, 0), 1, Z - 1)

    def z_inside(z):
        face, below = pl.ds(z, 1), pl.ds(z - 1, 1)
        for low, count in ((0, quarter), (quarter, Y - quarter)):
            cols = pl.ds(low, count)
            fz[face, cols] = between(vz, (face, cols), (below, cols), (face, cols))
    loop(1, Z, z_inside)
    for copy in z_flux:
        copy.wait()
    fz[pl.ds(0, 1)] = fz[pl.ds(0, 1)] + fz_in[0]
    fz[pl.ds(Z, 1)] = fz[pl.ds(Z, 1)] + fz_in[1]

    def z_update(z):
        for y in range(Y):
            value = (g2[z + 1, y + 1] - fz[z + 1, y] + fz[z, y]) / (
                1.0 - step_value * vz[z + 1, y] + step_value * vz[z, y]
            )
            out_ref[z, pl.ds(y, T, stride=Y), :] = value
    loop(0, Z, z_update)


def solution(mesh):
    n_gy, n_gz = mesh.shape["gy"], mesh.shape["gz"]

    def shards(*blocks):
        Z, Y, X = blocks[0].shape
        T = X // LANES

        def split(block):
            return block.reshape(Z, Y, T, LANES).transpose(0, 2, 1, 3).reshape(Z, T * Y, LANES)

        def rows(*lead):
            return pltpu.VMEM((*lead, T, LANES), jnp.float32)

        dma = pltpu.SemaphoreType.DMA
        padded = rows(Z + 2, Y + 2)
        plain = rows(Z, Y)
        field, dt = pl.pallas_call(
            functools.partial(kernel, n_gy, n_gz),
            out_shape=(
                jax.ShapeDtypeStruct((Z, T * Y, LANES), jnp.float32),
                jax.ShapeDtypeStruct((1, 1), jnp.float32),
            ),
            in_specs=[pl.BlockSpec(memory_space=pltpu.HBM)] * 4,
            out_specs=(
                pl.BlockSpec(memory_space=pltpu.VMEM),
                pl.BlockSpec(memory_space=pltpu.SMEM),
            ),
            scratch_shapes=[
                *[pltpu.VMEM((Z, T * Y, LANES), jnp.float32)] * 4, dma((4,)),
                padded, padded, padded, padded, padded,
                plain, plain, plain, plain,
                plain, rows(Z, Y + 1), rows(Z + 1, Y), rows(Z, Y + 1), rows(Z + 1, Y),
                rows(2, Z, 1), rows(2, 1, Y), rows(n_gy), rows(n_gz),
                dma((3, 8)), dma((3, 8)), dma((2,)), dma((2,)), dma((2, 2)), dma((2, 2)),
                dma((n_gy - 1,)), dma((n_gy - 1,)), dma((n_gz - 1,)), dma((n_gz - 1,)),
            ],
            compiler_params=pltpu.CompilerParams(
                collective_id=0, has_side_effects=True, vmem_limit_bytes=67043328
            ),
        )(*[split(block) for block in blocks])
        field = field.reshape(Z, T, Y, LANES).transpose(0, 2, 1, 3).reshape(Z, Y, X)
        return field, dt.reshape(())

    spec = P("gz", "gy", None)
    return jax.shard_map(
        shards, mesh=mesh, in_specs=(spec,) * 4, out_specs=(spec, P()), check_vma=False
    )
```
